32 devices in a mesh: groups: 2 (over y), ctx: 4 (over z), head: 4 (over x, core).
Axes of the slice: x: 2, y: 2, z: 4, core: 2. Of those that a mesh axis runs over, the one named last changes fastest.
Arguments:
- queries: bfloat16 [2048, 4096], P(('groups', 'ctx'), 'head'), parts along dimension 0, may hold values from -250 to 250
- rotated_key_rows: bfloat16 [2048, 1024], P(('groups', 'ctx'), 'head'), parts along dimension 0, may hold values from -6 to 6
- value_state_rows: bfloat16 [2048, 1024], P(('groups', 'ctx'), 'head'), parts along dimension 0, may hold values from -6 to 6
- retained_positions: int32 [8, 32], P(('groups', 'ctx')), parts along dimension 0, may hold values from 0 to 255, as said below
- anchor_length: int32 [2], P('groups'), parts along dimension 0, may hold values from 1 to 128
- out_proj: bfloat16 [4096, 4096], P('head'), may hold values from -0.125 to 0.125
Outputs:
- attn_out: bfloat16 [2048, 4096], P(('groups', 'ctx'), 'head'), parts along dimension 0
The draws below stay inside these ranges and needn't reach their ends.
There are 2 independent parts, one for each index of `groups`. The reference program is written for one: setup_inputs(seed, part) draws one part's arguments, and reference() takes and returns one part's arrays. A program takes and returns all parts, laid end to end along the dimension named above; an argument that names none is the same for every part. Nothing has to cross between parts.
Inputs may be any that keep to these rules, and one draw needn't show every extreme that they name: `retained_positions`: each row holds 32 different positions in increasing order.
All inputs are finite; a program needn't handle non-finite values.
Results may differ from the reference program's by a relative error of at most 0.015.
Values may be sent and summed in bfloat16 or wider, within the bound.
No kernel may reach another device: no remote copies, remote signals or barrier semaphores. Data moves between devices by JAX's collectives and lax.ppermute only.
A program may use at most 64 MiB of HBM per device.

```python
import jax
import jax.numpy as jnp
from jax import lax

D = 4096
QUERY_HEADS = 32
KEY_VALUE_HEADS = 8
HEAD_SIZE = 128
BLOCK_TOKENS = 256
ANCHOR = 128
RETAINED_COUNT = 32
DOCUMENT_TOKENS = 1024
N_CTX = 4
N_HEAD = 4


def draw_queries(key, part):
    noise_key = jax.random.fold_in(jax.random.fold_in(key, 11), 0)
    sample = jax.random.normal(noise_key, (DOCUMENT_TOKENS, QUERY_HEADS * HEAD_SIZE), jnp.float32)
    return jnp.clip(sample, -6.0, 6.0).astype(jnp.bfloat16)


def draw_retained_positions(key, part):
    row_keys = jax.random.split(jax.random.fold_in(key, 23), N_CTX)
    orders = jax.vmap(lambda row_key: jax.random.permutation(row_key, BLOCK_TOKENS))(row_keys)
    return jnp.sort(orders[:, :RETAINED_COUNT].astype(jnp.int32), axis=1)


def with_spikes(entries, own_key, source, target, parts, factor):
    owner, partner = [(jnp.arange(entries.shape[dim]) // (entries.shape[dim] // parts)).reshape([-1 if axis == dim else 1 for axis in range(entries.ndim)]) for dim in (source, target)]
    chosen = jax.random.permutation(own_key, parts)[partner]
    strong = (owner == chosen) | (owner == (partner + parts // 2) % parts)
    return jnp.where(strong, factor * entries, entries)


def block_levels(own_key, shape, cuts, smallest, top_value):
    factor_of = 1.0
    for dim, blocks in cuts:
        steps = jax.random.uniform(jax.random.fold_in(jax.random.fold_in(own_key, 6), dim), (blocks,), jnp.float32, smallest / len(cuts), top_value / len(cuts))
        factor_of = factor_of * jnp.repeat(jnp.exp(steps), shape[dim] // blocks).reshape((-1,) + (1,) * (len(shape) - 1 - dim))
    return factor_of


def gaussian(rng, extent, spread, reach, cuts=(), kind=jnp.bfloat16):
    values = spread * jax.random.normal(rng, extent, jnp.float32)
    if cuts:
        values = values * block_levels(rng, extent, cuts, -0.22, 0.18)
    return jnp.clip(values, -reach, reach).astype(kind)


def gaussian_with(own_key, extent, spread, reach, cuts, heavy, kind=jnp.bfloat16):
    array = spread * jax.random.normal(own_key, extent, jnp.float32)
    if cuts:
        array = array * block_levels(own_key, extent, cuts, -0.22, 0.18)
    return jnp.clip(with_spikes(array, jax.random.fold_in(own_key, 3), *heavy), -reach, reach).astype(kind)


def setup_inputs(seed: int = 0, part: int = 0) -> dict:
    streams_of = jax.random.split(jax.random.key(seed), 7)
    part_keys = jax.random.split(jax.random.fold_in(streams_of[6], part), 7)
    return {
        "queries": draw_queries(jax.random.fold_in(jax.random.fold_in(streams_of[6], part), 71), part),
        "rotated_key_rows": gaussian(part_keys[1], (DOCUMENT_TOKENS, KEY_VALUE_HEADS * HEAD_SIZE), 1.0, 6.0, ((0, 4), (1, 4))),
        "value_state_rows": gaussian(part_keys[2], (DOCUMENT_TOKENS, KEY_VALUE_HEADS * HEAD_SIZE), 1.0, 6.0, ((0, 4), (1, 4))),
        "retained_positions": draw_retained_positions(jax.random.fold_in(jax.random.fold_in(streams_of[6], part), 71), part),
        "anchor_length": jax.random.randint(part_keys[4], (1,), 1, ANCHOR + 1).astype(jnp.int32),
        "out_proj": gaussian_with(streams_of[5], (QUERY_HEADS * HEAD_SIZE, D), (QUERY_HEADS * HEAD_SIZE) ** -0.5, 0.125, ((0, 4),), (0, 1, 4, 2.0)),
    }


def reference(queries, rotated_key_rows, value_state_rows, retained_positions, anchor_length, out_proj):
    queries_per_key_head = QUERY_HEADS // KEY_VALUE_HEADS
    inv_root = HEAD_SIZE ** -0.5
    query_head_rows = queries.reshape(N_CTX, BLOCK_TOKENS, KEY_VALUE_HEADS, queries_per_key_head, HEAD_SIZE)
    key_head_rows = rotated_key_rows.reshape(N_CTX, BLOCK_TOKENS, KEY_VALUE_HEADS, HEAD_SIZE)
    value_head_rows = value_state_rows.reshape(N_CTX, BLOCK_TOKENS, KEY_VALUE_HEADS, HEAD_SIZE)
    block_indices = jnp.arange(N_CTX, dtype=jnp.int32)[:, None]
    passing_key_rows = key_head_rows[block_indices, retained_positions].reshape(N_CTX * RETAINED_COUNT, KEY_VALUE_HEADS, HEAD_SIZE)
    passing_value_rows = value_head_rows[block_indices, retained_positions].reshape(N_CTX * RETAINED_COUNT, KEY_VALUE_HEADS, HEAD_SIZE)
    anchor_keys = key_head_rows[0, :ANCHOR]
    anchor_vals = value_head_rows[0, :ANCHOR]
    places = jnp.arange(BLOCK_TOKENS, dtype=jnp.int32)

    def one_host(host_id):
        all_keys = jnp.concatenate([anchor_keys, passing_key_rows, key_head_rows[host_id]], axis=0)
        all_vals = jnp.concatenate([anchor_vals, passing_value_rows, value_head_rows[host_id]], axis=0)
        anchor_ok = (jnp.arange(ANCHOR, dtype=jnp.int32) < anchor_length[0]) & (host_id > 0)
        passed_ok = jnp.arange(N_CTX * RETAINED_COUNT, dtype=jnp.int32) // RETAINED_COUNT < host_id
        allowed = jnp.concatenate([
            jnp.broadcast_to(anchor_ok[None, :], (BLOCK_TOKENS, ANCHOR)),
            jnp.broadcast_to(passed_ok[None, :], (BLOCK_TOKENS, N_CTX * RETAINED_COUNT)),
            places[None, :] <= places[:, None]], axis=1)
        scores = jnp.einsum("tkgd,nkd->kgtn", query_head_rows[host_id].astype(jnp.float32),
                            all_keys.astype(jnp.float32), precision=lax.Precision.HIGHEST) * inv_root
        scores = jnp.where(allowed, scores, -1e30)
        maxima = jnp.max(scores, axis=-1, keepdims=True)
        weights = jnp.where(allowed, jnp.exp(scores - maxima), 0.0)
        totals = jnp.sum(weights, axis=-1)
        rounded = lax.optimization_barrier(weights.astype(jnp.bfloat16)).astype(jnp.float32)
        numerator = jnp.einsum("kgtn,nkd->kgtd", rounded, all_vals.astype(jnp.float32),
                               precision=lax.Precision.HIGHEST)
        result = numerator / totals[..., None]
        return result.transpose(2, 0, 1, 3).reshape(BLOCK_TOKENS, QUERY_HEADS * HEAD_SIZE).astype(jnp.bfloat16)

    attended = lax.map(one_host, jnp.arange(N_CTX, dtype=jnp.int32)).reshape(DOCUMENT_TOKENS, QUERY_HEADS * HEAD_SIZE)
    slab_width = QUERY_HEADS * HEAD_SIZE // N_HEAD
    head_outs = attended.reshape(DOCUMENT_TOKENS, N_HEAD, slab_width).transpose(1, 0, 2)
    head_weights = out_proj.reshape(N_HEAD, slab_width, D)

    def accumulate(running, pieces):
        partial_value = jnp.dot(pieces[0], pieces[1], preferred_element_type=jnp.float32)
        partial_value = lax.optimization_barrier(partial_value.astype(jnp.bfloat16)).astype(jnp.float32)
        return running + partial_value, None

    summed, unused = lax.scan(accumulate, jnp.zeros((DOCUMENT_TOKENS, D), jnp.float32), (head_outs, head_weights))
    return summed.astype(jnp.bfloat16)
```

```python
import functools

import jax
import jax.numpy as jnp
from jax import lax
from jax.sharding import PartitionSpec as P

HEAD_SIZE = 128
ANCHOR = 128
RETAINED_COUNT = 32


def context_rows(keys, values, positions, n):
    me = lax.axis_index("ctx")
    first = jnp.concatenate([keys[:ANCHOR], values[:ANCHOR]], axis=1)
    own = jnp.concatenate([keys, values], axis=1)
    chosen = (positions[:, None] == jnp.arange(own.shape[0], dtype=jnp.int32)[None, :]).astype(own.dtype)
    kept = jnp.dot(chosen, own, preferred_element_type=jnp.float32).astype(own.dtype)
    both = jnp.concatenate([first, kept], axis=0)
    anchor, passed = 0, []
    for shift in range(1, n):
        near = lax.ppermute(both, "ctx", [(0, shift)])
        rest = [(i, i + shift) for i in range(1, n - shift)]
        other = lax.ppermute(kept, "ctx", rest) if rest else jnp.zeros_like(kept)
        anchor = jnp.where(me == shift, near[:ANCHOR], anchor)
        passed.append(jnp.where(me == shift, near[ANCHOR:], other))
    return anchor, jnp.concatenate(passed, axis=0)


def scatter_sum(partial, n):
    me = lax.axis_index("head")
    bit = 1
    width = partial.shape[1] // n
    held = {0: partial}
    blocks = {o: lax.dynamic_slice_in_dim(partial, (me ^ o) * width, width, 1) for o in range(n)}
    while bit < n:
        pairs = [(i, i ^ bit) for i in range(n)]
        kept = {}
        for o in sorted(blocks, reverse=True):
            if o & bit:
                got = lax.ppermute(blocks[o].astype(jnp.bfloat16), "head", pairs)
                kept[o ^ bit] = blocks[o ^ bit].astype(jnp.float32) + got.astype(jnp.float32)
        blocks = kept
        bit *= 2
    return blocks[0].astype(jnp.bfloat16)


def local(queries, rotated_key_rows, value_state_rows, retained_positions, anchor_length, out_proj, *, n_ctx, n_head):
    tok_rows = queries.shape[0]
    kv_heads = rotated_key_rows.shape[1] // HEAD_SIZE
    queries_per_key_head = queries.shape[1] // rotated_key_rows.shape[1]
    inv_root = HEAD_SIZE ** (-0.5)
    my_host = lax.axis_index("ctx")
    heads_q = queries.reshape(tok_rows, kv_heads, queries_per_key_head, HEAD_SIZE)
    places = jnp.arange(tok_rows, dtype=jnp.int32)

    def absorb(running, key_rows, val_rows, allowed):
        maxima, totals, numerator = running
        key_count = key_rows.shape[0]
        key_heads = key_rows.reshape(key_count, kv_heads, HEAD_SIZE)
        val_heads = val_rows.reshape(key_count, kv_heads, HEAD_SIZE)
        scores = (
            jnp.einsum("tkgd,nkd->kgtn", heads_q, key_heads, preferred_element_type=jnp.float32)
            * inv_root
        )
        scores = jnp.where(allowed, scores, -1e30)
        new_max = jnp.maximum(maxima, jnp.max(scores, axis=-1))
        weights = jnp.where(allowed, jnp.exp(scores - new_max[..., None]), 0.0)
        rescale = jnp.exp(maxima - new_max)
        totals = totals * rescale + jnp.sum(weights, axis=-1)
        numerator = numerator * rescale[..., None] + jnp.einsum(
            "kgtn,nkd->kgtd",
            weights.astype(jnp.bfloat16),
            val_heads,
            preferred_element_type=jnp.float32,
        )
        return (new_max, totals, numerator)

    running = (
        jnp.full((kv_heads, queries_per_key_head, tok_rows), -1e30, jnp.float32),
        jnp.zeros((kv_heads, queries_per_key_head, tok_rows), jnp.float32),
        jnp.zeros((kv_heads, queries_per_key_head, tok_rows, HEAD_SIZE), jnp.float32),
    )
    anchor, passed = context_rows(rotated_key_rows, value_state_rows, retained_positions[0], n_ctx)
    width = rotated_key_rows.shape[1]
    anchor_keys, anchor_vals = anchor[:, :width], anchor[:, width:]
    anchor_ok = ((jnp.arange(ANCHOR, dtype=jnp.int32) < anchor_length[0]) & (my_host > 0))[None, :]
    running = absorb(running, anchor_keys, anchor_vals, anchor_ok)
    passing_key_rows, passing_value_rows = passed[:, :width], passed[:, width:]
    allowed = (jnp.arange(passed.shape[0], dtype=jnp.int32) // RETAINED_COUNT < my_host)[None, :]
    running = absorb(running, passing_key_rows, passing_value_rows, allowed)
    local_ok = places[None, :] <= places[:, None]
    running = absorb(running, rotated_key_rows, value_state_rows, local_ok)
    maxima, totals, numerator = running
    attended = (
        (numerator / totals[..., None])
        .transpose(2, 0, 1, 3)
        .reshape(tok_rows, -1)
        .astype(jnp.bfloat16)
    )
    partial_value = jnp.dot(attended, out_proj, preferred_element_type=jnp.float32)
    return scatter_sum(partial_value, n_head)
def solution(mesh):
    placed = (
        P(("groups", "ctx"), "head"),
        P(("groups", "ctx"), "head"),
        P(("groups", "ctx"), "head"),
        P(("groups", "ctx"), None),
        P("groups"),
        P("head", None),
    )
    body = functools.partial(local, n_ctx=mesh.shape["ctx"], n_head=mesh.shape["head"])
    return jax.shard_map(
        body, mesh=mesh, in_specs=placed, out_specs=P(("groups", "ctx"), "head"), check_vma=False
    )
```

```python
import functools

import jax
import jax.numpy as jnp
from jax import lax
from jax.experimental import pallas as pl
from jax.experimental.pallas import tpu as pltpu
from jax.sharding import PartitionSpec as P

HEAD_SIZE = 128
ANCHOR = 128
RETAINED_COUNT = 32
ROWS = 128
LOG2E = 1.4426950408889634
FACTOR = HEAD_SIZE ** (-0.5) * LOG2E
NEVER = -1e30
F32 = jnp.float32
BF16 = jnp.bfloat16
WHOLE = pl.BlockSpec(memory_space=pltpu.VMEM)
SCALARS = pl.BlockSpec(memory_space=pltpu.SMEM)
IN_PLACE = pl.BlockSpec(memory_space=pltpu.HBM)


def dot_rows(a, b):
    return lax.dot_general(a, b, (((1,), (1,)), ((), ())), preferred_element_type=F32)


def grant(mib):
    return pltpu.CompilerParams(vmem_limit_bytes=mib << 20)


def cost(flops, moved, exps=0):
    return pl.CostEstimate(flops=flops, bytes_accessed=moved, transcendentals=exps)


def start_all(moves, sems):
    copies = [pltpu.make_async_copy(src, dst, sems.at[i]) for i, (src, dst) in enumerate(moves)]
    for c in copies:
        c.start()
    return copies


def prepare_kernel(pos_hbm, k_hbm, v_hbm, out_ref, k_ref, v_ref, pos_ref, sems):
    copies = start_all([(pos_hbm, pos_ref), (k_hbm, k_ref), (v_hbm, v_ref)], sems)
    tokens, width = k_ref.shape
    rows = lax.broadcasted_iota(jnp.int32, (tokens, RETAINED_COUNT), 0)
    copies[0].wait()
    chosen = jnp.where(rows == pos_ref[...], 1.0, 0.0).astype(BF16)
    for at, ref, c in ((0, k_ref, copies[1]), (width, v_ref, copies[2])):
        c.wait()
        out_ref[:ANCHOR, at : at + width] = ref[:ANCHOR]
        kept = lax.dot_general(chosen, ref[...], (((0,), (0,)), ((), ())), preferred_element_type=F32)
        out_ref[ANCHOR:, at : at + width] = kept.astype(BF16)


def local_kernel(info_ref, q_hbm, k_ref, v_ref, w_hbm, num_ref, max_ref, sum_ref, q_ref, *rest):
    *weights, sems = rest
    cols = weights[0].shape[1]
    moves = [(q_hbm, q_ref)]
    for o, ref in enumerate(weights):
        at = pl.multiple_of((info_ref[2] ^ o) * cols, 128)
        moves.append((w_hbm.at[:, pl.ds(at, cols)], ref))
    copies = start_all(moves, sems)
    copies[0].wait()
    tokens = q_ref.shape[0]
    heads = q_ref.shape[1] // HEAD_SIZE
    group = q_ref.shape[1] // k_ref.shape[1]
    lane = lax.broadcasted_iota(jnp.int32, (ROWS, 128), 1)
    for top in range(0, tokens, ROWS):
        keys = top + ROWS
        row = lax.broadcasted_iota(jnp.int32, (ROWS, keys), 0) + top
        col = lax.broadcasted_iota(jnp.int32, (ROWS, keys), 1)
        seen = col <= row
        maxima = jnp.zeros((ROWS, 128), F32)
        totals = jnp.zeros((ROWS, 128), F32)
        for h in range(heads):
            at = h * HEAD_SIZE
            kat = (h // group) * HEAD_SIZE
            s = dot_rows(q_ref[top:keys, at : at + HEAD_SIZE], k_ref[:keys, kat : kat + HEAD_SIZE])
            s = jnp.where(seen, s, NEVER)
            m = jnp.max(s, axis=1, keepdims=True)
            p = jnp.exp2((s - m) * FACTOR)
            z = jnp.sum(p, axis=1, keepdims=True)
            num_ref[top:keys, at : at + HEAD_SIZE] = jnp.dot(
                p.astype(BF16), v_ref[:keys, kat : kat + HEAD_SIZE], preferred_element_type=F32
            )
            maxima = jnp.where(lane == h, m, maxima)
            totals = jnp.where(lane == h, z, totals)
        max_ref[top:keys, :] = maxima
        sum_ref[top:keys, :] = totals
    for c in copies[1:]:
        c.wait()


def multiply(att_ref, w_ref, part_ref):
    for top in range(0, part_ref.shape[0], ROWS):
        rows = slice(top, top + ROWS)
        part = jnp.dot(att_ref[rows, :], w_ref[...], preferred_element_type=F32)
        part_ref[rows, :] = part.astype(BF16)


def remote_kernel(info_ref, q_ref, far_ref, num_ref, max_ref, sum_ref, w_ref, att_ref, part_ref):
    tokens = q_ref.shape[0]
    heads = q_ref.shape[1] // HEAD_SIZE
    count, twice = far_ref.shape
    width = twice // 2
    group = q_ref.shape[1] // width
    index = lax.broadcasted_iota(jnp.int32, (1, count), 1)
    mine = info_ref[0]
    limit = jnp.where(mine > 0, info_ref[1], 0)
    seen = index < jnp.where(index < ANCHOR, limit, ANCHOR + mine * RETAINED_COUNT)
    for top in range(0, tokens, ROWS):
        rows = slice(top, top + ROWS)
        for h in range(heads):
            cols = slice(h * HEAD_SIZE, (h + 1) * HEAD_SIZE)
            kat = (h // group) * HEAD_SIZE
            s = dot_rows(q_ref[rows, cols], far_ref[:, kat : kat + HEAD_SIZE])
            s = jnp.where(seen, s, NEVER)
            before = max_ref[rows, h : h + 1]
            m = jnp.maximum(before, jnp.max(s, axis=1, keepdims=True))
            p = jnp.exp2((s - m) * FACTOR)
            scale = jnp.exp2((before - m) * FACTOR)
            z = sum_ref[rows, h : h + 1] * scale + jnp.sum(p, axis=1, keepdims=True)
            o = jnp.dot(
                p.astype(BF16), far_ref[:, width + kat : width + kat + HEAD_SIZE], preferred_element_type=F32
            )
            o = (num_ref[rows, cols] * scale + o) / z
            att_ref[rows, cols] = o.astype(BF16)
    multiply(att_ref, w_ref, part_ref)


def context_rows(message, n):
    me = lax.axis_index("ctx")
    kept = message[ANCHOR:]
    anchor, passed = 0, []
    for shift in range(1, n):
        last = n - 1 - shift
        pairs = [(0, shift)] + ([(last, n - 1)] if last > 0 else [])
        near = lax.ppermute(message, "ctx", pairs)
        rest = [(i, i + shift) for i in range(1, last)]
        block = near[ANCHOR:]
        if rest:
            other = lax.ppermute(kept, "ctx", rest)
            block = jnp.where((me == shift) | (me == n - 1), block, other)
        anchor = jnp.where(me == shift, near[:ANCHOR], anchor)
        passed.append(block)
    passed.append(jnp.zeros_like(kept))
    return jnp.concatenate([anchor] + passed, axis=0)


def local(queries, keys, values, positions, anchor_length, out_proj, *, n_ctx, n_head):
    tokens, model = queries.shape
    width = keys.shape[1]
    heads = model // HEAD_SIZE
    cols = out_proj.shape[1] // n_head
    depth = out_proj.shape[0]
    my_ctx = lax.axis_index("ctx")
    my_head = lax.axis_index("head")

    info = jnp.stack([my_ctx, anchor_length[0], my_head]).astype(jnp.int32)
    fixed = [pltpu.with_memory_space_constraint(x, pltpu.HBM) for x in (positions, keys, values, queries, out_proj)]
    positions, keys, values, queries, out_proj = fixed
    message, keys, values = pl.pallas_call(
        prepare_kernel,
        out_shape=[
            jax.ShapeDtypeStruct((ANCHOR + RETAINED_COUNT, 2 * width), BF16),
            jax.ShapeDtypeStruct(keys.shape, BF16),
            jax.ShapeDtypeStruct(values.shape, BF16),
        ],
        in_specs=[IN_PLACE] * 3,
        out_specs=[WHOLE] * 3,
        scratch_shapes=[pltpu.VMEM(positions.shape, jnp.int32), pltpu.SemaphoreType.DMA((3,))],
        compiler_params=grant(4),
        cost_estimate=cost(2 * tokens * RETAINED_COUNT * width * 2, tokens * width * 4),
    )(positions, keys, values)
    far = context_rows(message, n_ctx)

    num, maxima, totals, queries, *weights = pl.pallas_call(
        local_kernel,
        out_shape=[
            jax.ShapeDtypeStruct((tokens, model), F32),
            jax.ShapeDtypeStruct((tokens, 128), F32),
            jax.ShapeDtypeStruct((tokens, 128), F32),
            jax.ShapeDtypeStruct((tokens, model), BF16),
        ]
        + [jax.ShapeDtypeStruct((depth, cols), BF16)] * n_head,
        in_specs=[SCALARS, IN_PLACE, WHOLE, WHOLE, IN_PLACE],
        out_specs=[WHOLE] * (4 + n_head),
        scratch_shapes=[pltpu.SemaphoreType.DMA((1 + n_head,))],
        compiler_params=grant(24),
        cost_estimate=cost(4 * tokens * tokens * model, tokens * model * 6, heads * tokens * tokens),
    )(info, queries, keys, values, out_proj)

    part_shape = jax.ShapeDtypeStruct((tokens, cols), BF16)
    count = far.shape[0]
    attended, part = pl.pallas_call(
        remote_kernel,
        out_shape=[jax.ShapeDtypeStruct((tokens, model), BF16), part_shape],
        in_specs=[SCALARS] + [WHOLE] * 6,
        out_specs=[WHOLE] * 2,
        compiler_params=grant(12),
        cost_estimate=cost(
            4 * tokens * count * model + 2 * tokens * depth * cols, depth * cols * 2, heads * tokens * count
        ),
    )(info, queries, far, num, maxima, totals, weights[n_head - 1])

    def project(offset):
        return pl.pallas_call(
            multiply,
            out_shape=part_shape,
            in_specs=[WHOLE, WHOLE],
            out_specs=WHOLE,
            compiler_params=grant(8),
            cost_estimate=cost(2 * tokens * depth * cols, depth * cols * 2),
        )(attended, weights[offset])

    blocks = {o: part if o == n_head - 1 else project(o) for o in range(n_head - 1, -1, -1)}
    bit = 1
    while bit < n_head:
        pairs = [(i, i ^ bit) for i in range(n_head)]
        kept = {}
        for o in sorted(blocks, reverse=True):
            if o & bit:
                got = lax.ppermute(blocks[o], "head", pairs)
                kept[o ^ bit] = (blocks[o ^ bit].astype(F32) + got.astype(F32)).astype(BF16)
        blocks = kept
        bit *= 2
    return blocks[0]


def solution(mesh):
    placed = (
        P(("groups", "ctx"), "head"),
        P(("groups", "ctx"), "head"),
        P(("groups", "ctx"), "head"),
        P(("groups", "ctx"), None),
        P("groups"),
        P("head", None),
    )
    body = functools.partial(local, n_ctx=mesh.shape["ctx"], n_head=mesh.shape["head"])
    return jax.shard_map(
        body, mesh=mesh, in_specs=placed, out_specs=P(("groups", "ctx"), "head"), check_vma=False
    )
```

```python
import functools

import jax
import jax.numpy as jnp
from jax import lax
from jax.experimental import pallas as pl
from jax.experimental.pallas import tpu as pltpu
from jax.sharding import PartitionSpec as P


HEAD_SIZE = 128
ANCHOR = 128
RETAINED_COUNT = 32
ROWS = 128
CHUNKS = 2
LOG2E = 1.4426950408889634
FACTOR = HEAD_SIZE ** (-0.5) * LOG2E
NEVER = -1e30
F32 = jnp.float32
BF16 = jnp.bfloat16
WHOLE = pl.BlockSpec(memory_space=pltpu.VMEM)
SCALARS = pl.BlockSpec(memory_space=pltpu.SMEM)
IN_PLACE = pl.BlockSpec(memory_space=pltpu.HBM)


def dot_rows(a, b):
    return lax.dot_general(a, b, (((1,), (1,)), ((), ())), preferred_element_type=F32)


def grant(mib):
    return pltpu.CompilerParams(vmem_limit_bytes=mib << 20)


def cost(flops, moved, exps=0):
    return pl.CostEstimate(flops=flops, bytes_accessed=moved, transcendentals=exps)


def start_all(moves, sems):
    copies = [pltpu.make_async_copy(src, dst, sems.at[i]) for i, (src, dst) in enumerate(moves)]
    for c in copies:
        c.start()
    return copies


def prepare_kernel(pos_hbm, k_hbm, v_hbm, out_ref, k_ref, v_ref, pos_ref, sems):
    copies = start_all([(pos_hbm, pos_ref), (k_hbm, k_ref), (v_hbm, v_ref)], sems)
    tokens, width = k_ref.shape
    rows = lax.broadcasted_iota(jnp.int32, (tokens, RETAINED_COUNT), 0)
    copies[0].wait()
    chosen = jnp.where(rows == pos_ref[...], 1.0, 0.0).astype(BF16)
    for at, ref, c in ((0, k_ref, copies[1]), (width, v_ref, copies[2])):
        c.wait()
        out_ref[:ANCHOR, at : at + width] = ref[:ANCHOR]
        kept = lax.dot_general(chosen, ref[...], (((0,), (0,)), ((), ())), preferred_element_type=F32)
        out_ref[ANCHOR:, at : at + width] = kept.astype(BF16)


def tile(x, t):
    return x[:, t * HEAD_SIZE : (t + 1) * HEAD_SIZE]


def weigh(s, m):
    parts = [jnp.exp2((tile(s, t) - m) * FACTOR) for t in range(s.shape[1] // HEAD_SIZE)]
    return jnp.concatenate(parts, axis=1).astype(BF16)


def with_ones(v):
    return jnp.concatenate([v, jnp.ones_like(v)], axis=1)


def local_kernel(info_ref, q_hbm, k_ref, v_ref, w_hbm, num_ref, max_ref, sum_ref, q_ref, *rest):
    *weights, s_ref, p_ref, sems = rest
    cols = weights[0].shape[1]
    moves = [(q_hbm, q_ref)]
    for o, ref in enumerate(weights):
        at = pl.multiple_of((info_ref[2] ^ o) * cols, 128)
        moves.append((w_hbm.at[:, pl.ds(at, cols)], ref))
    copies = start_all(moves, sems)
    copies[0].wait()
    tokens = q_ref.shape[0]
    heads = q_ref.shape[1] // HEAD_SIZE
    group = q_ref.shape[1] // k_ref.shape[1]
    for top in range(0, tokens, ROWS):
        rows, keys = slice(top, top + ROWS), top + ROWS
        row = lax.broadcasted_iota(jnp.int32, (ROWS, keys), 0) + top
        col = lax.broadcasted_iota(jnp.int32, (ROWS, keys), 1)
        seen = col <= row
        for h in range(heads):
            s = dot_rows(tile(q_ref[rows, :], h), tile(k_ref[:keys, :], h // group))
            s_ref[h, :, :keys] = jnp.where(seen, s, NEVER)
        for h in range(heads):
            s = s_ref[h, :, :keys]
            m = jnp.broadcast_to(jnp.max(s, axis=1, keepdims=True), (ROWS, HEAD_SIZE))
            max_ref[rows, h * HEAD_SIZE : (h + 1) * HEAD_SIZE] = m
            p_ref[h, :, :keys] = weigh(s, m)
        for h in range(heads):
            at = slice(h * HEAD_SIZE, (h + 1) * HEAD_SIZE)
            both = jnp.dot(
                p_ref[h, :, :keys], with_ones(tile(v_ref[:keys, :], h // group)), preferred_element_type=F32
            )
            num_ref[rows, at] = tile(both, 0)
            sum_ref[rows, at] = tile(both, 1)
    for c in copies[1:]:
        c.wait()


def multiply(*refs):
    *att_refs, w_ref, part_ref = refs
    at = 0
    for att_ref in att_refs:
        for top in range(0, att_ref.shape[0], ROWS):
            part = jnp.dot(att_ref[top : top + ROWS, :], w_ref[...], preferred_element_type=F32)
            part_ref[at : at + ROWS, :] = part.astype(BF16)
            at += ROWS


def remote_kernel(
    start, info_ref, q_ref, far_ref, num_ref, max_ref, sum_ref, w_ref, att_ref, part_ref, s_ref, p_ref, m_ref
):
    heads = q_ref.shape[1] // HEAD_SIZE
    count, twice = far_ref.shape
    width = twice // 2
    group = q_ref.shape[1] // width
    index = lax.broadcasted_iota(jnp.int32, (1, count), 1)
    mine = info_ref[0]
    limit = jnp.where(mine > 0, info_ref[1], 0)
    seen = index < jnp.where(index < ANCHOR, limit, ANCHOR + mine * RETAINED_COUNT)
    for top in range(0, att_ref.shape[0], ROWS):
        rows, put = slice(start + top, start + top + ROWS), slice(top, top + ROWS)
        for h in range(heads):
            s = dot_rows(tile(q_ref[rows, :], h), tile(far_ref, h // group))
            s_ref[h] = jnp.where(seen, s, NEVER)
        for h in range(heads):
            at = slice(h * HEAD_SIZE, (h + 1) * HEAD_SIZE)
            s = s_ref[h]
            before = max_ref[rows, at]
            m = jnp.maximum(before, jnp.max(s, axis=1, keepdims=True))
            p_ref[h] = weigh(s, m)
            m_ref[:, at] = jnp.exp2((before - m) * FACTOR)
        for h in range(heads):
            at = slice(h * HEAD_SIZE, (h + 1) * HEAD_SIZE)
            both = jnp.dot(
                p_ref[h], with_ones(tile(far_ref, width // HEAD_SIZE + h // group)), preferred_element_type=F32
            )
            scale = m_ref[:, at]
            o = num_ref[rows, at] * scale + tile(both, 0)
            z = sum_ref[rows, at] * scale + tile(both, 1)
            att_ref[put, at] = (o / z).astype(BF16)
    multiply(att_ref, w_ref, part_ref)


def context_rows(message, n):
    me = lax.axis_index("ctx")
    near = [lax.ppermute(message, "ctx", [(0, shift)]) for shift in range(1, n)]
    kept = message[ANCHOR:]
    anchor, passed = 0, []
    for shift in range(1, n):
        first = near[shift - 1]
        block = first[ANCHOR:]
        rest = [(i, i + shift) for i in range(1, n - shift)]
        if rest:
            other = lax.ppermute(kept, "ctx", rest)
            block = jnp.where(me == shift, block, other)
        anchor = jnp.where(me == shift, first[:ANCHOR], anchor)
        passed.append(block)
    short = -(n - 1) * RETAINED_COUNT % HEAD_SIZE
    passed.append(jnp.zeros((short, kept.shape[1]), kept.dtype))
    return jnp.concatenate([anchor] + passed, axis=0)


def local(*args, n_ctx, n_head):
    return layer(*args, n_ctx, n_head)


def layer(queries, keys, values, positions, anchor_length, out_proj, n_ctx, n_head):
    tokens, model = queries.shape
    width = keys.shape[1]
    heads = model // HEAD_SIZE
    cols = out_proj.shape[1] // n_head
    depth = out_proj.shape[0]
    my_ctx = lax.axis_index("ctx")
    my_head = lax.axis_index("head")

    info = jnp.stack([my_ctx, anchor_length[0], my_head]).astype(jnp.int32)
    fixed = [pltpu.with_memory_space_constraint(x, pltpu.HBM) for x in (positions, keys, values, queries, out_proj)]
    positions, keys, values, queries, out_proj = fixed
    message, keys, values = pl.pallas_call(
        prepare_kernel,
        out_shape=[
            jax.ShapeDtypeStruct((ANCHOR + RETAINED_COUNT, 2 * width), BF16),
            jax.ShapeDtypeStruct(keys.shape, BF16),
            jax.ShapeDtypeStruct(values.shape, BF16),
        ],
        in_specs=[IN_PLACE] * 3,
        out_specs=[WHOLE] * 3,
        scratch_shapes=[pltpu.VMEM(positions.shape, jnp.int32), pltpu.SemaphoreType.DMA((3,))],
        compiler_params=grant(4),
        cost_estimate=cost(2 * tokens * RETAINED_COUNT * width * 2, tokens * width * 4),
    )(positions, keys, values)
    far = context_rows(message, n_ctx)

    num, maxima, totals, queries, *weights = pl.pallas_call(
        local_kernel,
        out_shape=[
            jax.ShapeDtypeStruct((tokens, model), F32),
            jax.ShapeDtypeStruct((tokens, model), F32),
            jax.ShapeDtypeStruct((tokens, model), F32),
            jax.ShapeDtypeStruct((tokens, model), BF16),
        ]
        + [jax.ShapeDtypeStruct((depth, cols), BF16)] * n_head,
        in_specs=[SCALARS, IN_PLACE, WHOLE, WHOLE, IN_PLACE],
        out_specs=[WHOLE] * (4 + n_head),
        scratch_shapes=[
            pltpu.VMEM((heads, ROWS, tokens), F32),
            pltpu.VMEM((heads, ROWS, tokens), BF16),
            pltpu.SemaphoreType.DMA((1 + n_head,)),
        ],
        compiler_params=grant(24),
        cost_estimate=cost(4 * tokens * tokens * model, tokens * model * 6, heads * tokens * tokens),
    )(info, queries, keys, values, out_proj)

    rows = tokens // CHUNKS
    count = far.shape[0]
    half = n_head // 2

    def attend(start, far):
        return pl.pallas_call(
            functools.partial(remote_kernel, start),
            out_shape=[jax.ShapeDtypeStruct((rows, model), BF16), jax.ShapeDtypeStruct((rows, cols), BF16)],
            in_specs=[SCALARS] + [WHOLE] * 6,
            out_specs=[WHOLE] * 2,
            scratch_shapes=[
                pltpu.VMEM((heads, ROWS, count), F32),
                pltpu.VMEM((heads, ROWS, count), BF16),
                pltpu.VMEM((ROWS, model), F32),
            ],
            compiler_params=grant(16),
            cost_estimate=cost(
                4 * rows * count * model + 2 * rows * depth * cols, depth * cols * 2, heads * rows * count
            ),
        )(info, queries, far, num, maxima, totals, weights[n_head - 1])

    def project(attended, offset):
        height = sum(a.shape[0] for a in attended)
        return pl.pallas_call(
            multiply,
            out_shape=jax.ShapeDtypeStruct((height, cols), BF16),
            in_specs=[WHOLE] * (len(attended) + 1),
            out_specs=WHOLE,
            compiler_params=grant(8),
            cost_estimate=cost(2 * height * depth * cols, depth * cols * 2),
        )(*attended, weights[offset])

    def exchange(block, bit):
        return lax.ppermute(block, "head", [(i, i ^ bit) for i in range(n_head)])

    def halve(blocks):
        bit = 1
        while bit < half:
            for o in sorted(blocks, reverse=True):
                if o & bit:
                    got = exchange(blocks.pop(o), bit)
                    blocks[o ^ bit] = (blocks[o ^ bit].astype(F32) + got.astype(F32)).astype(BF16)
            bit *= 2
        return blocks.popitem()[1]

    attended, crossed = [], []
    for c in range(CHUNKS):
        att, part = attend(c * rows, far)
        blocks = {o: project([att], o) for o in range(n_head - 2, half - 1, -1)}
        blocks[n_head - 1] = part
        total = halve(blocks)
        far, total, att = lax.optimization_barrier((far, total, att))
        attended.append(att)
        crossed.append(exchange(total, half))
    *attended, _ = lax.optimization_barrier((*attended, total))
    near = halve({o: project(attended, o) for o in range(half - 1, -1, -1)})
    return (near.astype(F32) + jnp.concatenate(crossed, axis=0).astype(F32)).astype(BF16)


def solution(mesh):
    placed = (
        P(("groups", "ctx"), "head"),
        P(("groups", "ctx"), "head"),
        P(("groups", "ctx"), "head"),
        P(("groups", "ctx"), None),
        P("groups"),
        P("head", None),
    )
    body = functools.partial(local, n_ctx=mesh.shape["ctx"], n_head=mesh.shape["head"])
    return jax.shard_map(
        body, mesh=mesh, in_specs=placed, out_specs=P(("groups", "ctx"), "head"), check_vma=False
    )
```
